32 devices in a mesh: rep: 4 (over x, core), row: 2 (over y), col: 4 (over z).
Axes of the slice: x: 2, y: 2, z: 4, core: 2. Of those that a mesh axis runs over, the one named last changes fastest.
Arguments:
- spin_init: bfloat16 [256, 8192], P('rep', 'row'), may hold values from -1 to 1, as said below
- couplings: bfloat16 [2, 4, 1024, 8192], P(None, 'col', None, 'row'), may hold values from -1 to 1, as said below
- flip_noise: float32 [10, 256, 8192], P(None, 'rep', 'row'), may hold values from 0 to 17, as said below
- colors: int32 [8192], P('row'), may hold values 0 or 1
- beta_steps: int32 [256], replicated, may hold values from 96 to 1024
- partners: int32 [256], replicated, may hold values from 0 to 255, as said below
- swap_noise: float32 [256], replicated, may hold values from 0 to 17, as said below
Outputs:
- spins_out: bfloat16 [256, 8192], P('rep', 'row')
- energies: float32 [256], P('rep')
The draws below stay inside these ranges and needn't reach their ends.
Inputs may be any that keep to these rules, and one draw needn't show every extreme that they name: `spin_init`: every entry is -1 or +1. `couplings`: the 8192 x 8192 matrix is symmetric, zero on its diagonal, and every other entry is -1 or +1. `flip_noise`: independent exponential variates of mean one. `swap_noise`: independent exponential variates of mean one. Pairs slots: partners[partners[r]] = r and partners[r] != r for every slot.
All inputs are finite; a program needn't handle non-finite values. No bound on the sum of `colors` on one device may be relied on, other than what follows from the above.
Results may differ from the reference program's by a relative error of at most 0.001.
Values may be sent and summed in bfloat16 or wider, within the bound.
A program may use at most 64 MiB of HBM per device.

```python
import math
import jax
import jax.numpy as jnp
from jax import lax

N = 8192
SWEEPS = 10
R = 256
PIECE = 1024
N_ROW = 2
N_COL = 4


def draw_spin_init(key, part):
    coin_flips = jax.random.randint(key, (R, N), 0, 2)
    return (coin_flips.astype(jnp.float32) * 2.0 - 1.0).astype(jnp.bfloat16)


def draw_couplings(key, part):
    coin_flips = jax.random.randint(key, (N, N), 0, 2).astype(jnp.float32) * 2.0 - 1.0
    row_ids = jnp.arange(N)[:, None]
    col_ids = jnp.arange(N)[None, :]
    symmetric = jnp.where(row_ids < col_ids, coin_flips, coin_flips.T)
    symmetric = jnp.where(row_ids == col_ids, 0.0, symmetric)
    return symmetric.astype(jnp.float32).reshape(N_ROW, N_COL, PIECE, N).astype(jnp.bfloat16)


def draw_flip_noise(key, part):
    return jax.random.exponential(key, (SWEEPS, R, N), jnp.float32)


def draw_swap_noise(key, part):
    return jax.random.exponential(key, (R,), jnp.float32)


def draw_partners(key, part):
    shuffled = jax.random.permutation(key, R).astype(jnp.int32)
    first_half = shuffled[0::2]
    second_half = shuffled[1::2]
    mate_table = jnp.zeros((R,), jnp.int32)
    mate_table = mate_table.at[first_half].set(second_half)
    mate_table = mate_table.at[second_half].set(first_half)
    return mate_table


def set_ends(drawn, rng, least, largest):
    place = [jax.random.randint(jax.random.fold_in(rng, axis), (), 0, length) for axis, length in enumerate(drawn.shape)]
    widest = drawn.shape.index(max(drawn.shape))
    neighbour = place[:widest] + [(place[widest] + 1) % drawn.shape[widest]] + place[widest + 1:]
    return drawn.at[tuple(place)].set(least).at[tuple(neighbour)].set(largest)


def setup_inputs(seed: int = 0) -> dict:
    seeds = jax.random.split(jax.random.key(seed), 8)
    return {
        "spin_init": draw_spin_init(jax.random.fold_in(seeds[7], 71), 0),
        "couplings": draw_couplings(jax.random.fold_in(seeds[7], 71), 0),
        "flip_noise": draw_flip_noise(jax.random.fold_in(seeds[7], 71), 0),
        "colors": set_ends((jax.random.randint(seeds[3], (N,), 0, 2) < 1).astype(jnp.int32), jax.random.fold_in(seeds[3], 1), 0, 1),
        "beta_steps": set_ends(jax.random.randint(seeds[4], (R,), 96, 1025), jax.random.fold_in(seeds[4], 1), 96, 1024).astype(jnp.int32),
        "partners": draw_partners(jax.random.fold_in(seeds[7], 71), 0),
        "swap_noise": draw_swap_noise(jax.random.fold_in(seeds[7], 71), 0),
    }


def reference(spin_init, couplings, flip_noise, colors, beta_steps, partners, swap_noise):
    matrix = couplings.reshape(N, N).astype(jnp.float32)
    spin_state = spin_init.astype(jnp.float32)
    beta_col = beta_steps.astype(jnp.float32)[:, None]
    for step_index in range(SWEEPS):
        fields = jnp.dot(spin_state, matrix, precision=lax.Precision.HIGHEST, preferred_element_type=jnp.float32)
        energy_cost = beta_col * (spin_state * fields) * (1.0 / 16384.0)
        flipped = (colors == step_index % 2)[None, :] & (energy_cost < flip_noise[step_index])
        spin_state = jnp.where(flipped, -spin_state, spin_state)
    fields = jnp.dot(spin_state, matrix, precision=lax.Precision.HIGHEST, preferred_element_type=jnp.float32)
    energy = -0.5 * lax.optimization_barrier(jnp.sum(spin_state * fields, axis=1))
    slot_ids = jnp.arange(R, dtype=jnp.int32)
    all_betas = beta_steps.astype(jnp.float32)
    mate_energy = energy[partners]
    swap_gain = (all_betas - all_betas[partners]) * (energy - mate_energy) * (1.0 / (64.0 * N * math.sqrt(N)))
    accept = swap_gain + swap_noise[jnp.minimum(slot_ids, partners)] > 0.0
    spins_out = jnp.where(accept[:, None], spin_state[partners], spin_state).astype(jnp.bfloat16)
    energies = jnp.where(accept, mate_energy, energy) * (1.0 / (N * math.sqrt(N)))
    return (spins_out, energies)
```

```python
import functools
import math

import jax
import jax.numpy as jnp
from jax import lax
from jax.experimental import pallas as pl
from jax.experimental.pallas import tpu as pltpu
from jax.sharding import PartitionSpec as P

GROUPS = 2
F8 = jnp.float8_e4m3fn
ARRIVAL = (1, 3, 2)


def metropolis(values, fields, parity, color_part, noise_part, beta_col):
    energy_cost = beta_col * (values * fields) * (1.0 / 16384.0)
    flipped = (color_part == parity) & (energy_cost < noise_part)
    return jnp.where(flipped, -values, values).astype(jnp.bfloat16)


def column_to_row(column, mask):
    return jnp.sum(jnp.where(mask, column, 0.0), axis=0, keepdims=True)


def picked(mask, row):
    return jnp.sum(jnp.where(mask, row, 0.0), axis=1, keepdims=True)


def kernel(
    sweeps, spin_count, couple_ref, init_ref, noise_ref, color_ref, beta_col_ref, beta_row_ref,
    partner_ref, swap_ref, out_ref, energy_ref,
    state, part, got, own, noise_buf, every, esend, erecv, esum,
    noise_sem, zs, zr, ys, yr, xs, xr, cs, cr, fs, fr, es, er,
):
    rep, row, col = lax.axis_index("rep"), lax.axis_index("row"), lax.axis_index("col")
    rep_dev = init_ref.shape[0]
    piece = couple_ref.shape[2]
    rows = rep_dev // GROUPS
    slots = beta_row_ref.shape[1]
    y_mate = 1 - row
    core_mate = rep + 1 - 2 * (rep % 2)
    x_mate = rep + 2 - 4 * (rep // 2)

    def at(**changes):
        return (changes.get("rep", rep), changes.get("row", row), changes.get("col", col))

    def z_of(step):
        return (col + step) % 4

    def remote(src, dst, send, recv, device):
        return pltpu.make_async_remote_copy(
            src_ref=src, dst_ref=dst, send_sem=send, recv_sem=recv,
            device_id=device, device_id_type=pl.DeviceIdType.MESH,
        )

    noise_copy = pltpu.make_async_copy(
        noise_ref.at[:, :, pl.ds(pl.multiple_of(col * piece, 128), piece)], noise_buf, noise_sem
    )
    noise_copy.start()

    partners = [at(row=y_mate), at(rep=core_mate), at(rep=x_mate)] + [at(col=z_of(d)) for d in ARRIVAL]
    barrier = pltpu.get_barrier_semaphore()
    for device in partners:
        pl.semaphore_signal(barrier, inc=1, device_id=device, device_id_type=pl.DeviceIdType.MESH)
    pl.semaphore_wait(barrier, len(partners))

    for g in range(GROUPS):
        for z in range(4):
            state[0, g, z] = init_ref[g * rows:(g + 1) * rows, z * piece:(z + 1) * piece]

    def z_copy(slot, g, step):
        return remote(
            state.at[slot, g, col], state.at[slot, g, col],
            zs.at[slot, g, step - 1], zr.at[slot, g, step - 1], at(col=z_of(step)),
        )

    def y_copy(slot, g):
        return remote(part.at[slot, g], got.at[slot, g], ys.at[slot, g], yr.at[slot, g], at(row=y_mate))

    def product(slot, g, z, half):
        return jnp.dot(
            state[slot, g, z].astype(F8), couple_ref[z, half], preferred_element_type=jnp.float32
        )

    def x_copy(g, z, lane):
        return remote(
            state.at[0, g, z], every.at[z, rep, g], xs.at[lane, g], xr.at[lane, g], at(rep=x_mate)
        )

    def c_copy(g, z, lane):
        return remote(
            state.at[0, g, z], every.at[z, rep, g], cs.at[lane, g], cr.at[lane, g], at(rep=core_mate)
        )

    def f_copy(g, z, lane):
        return remote(
            every.at[z, x_mate, g], every.at[z, x_mate, g], fs.at[lane, g], fr.at[lane, g],
            at(rep=core_mate),
        )

    def matmuls(slot, g, first, last):
        def share(step, lane):
            if last:
                z = z_of(step)
                x_copy(g, z, step).start()
                c_copy(g, z, step).start()

        share(0, 0)
        total = product(slot, g, col, y_mate)
        for step in ARRIVAL:
            if not first:
                z_copy(slot, g, 4 - step).wait_recv()
            share(step, step)
            total += product(slot, g, z_of(step), y_mate)
        part[slot, g] = total.astype(jnp.int32).astype(jnp.int16)
        y_copy(slot, g).start()
        total = product(slot, g, col, row)
        for step in ARRIVAL:
            total += product(slot, g, z_of(step), row)
        own[g] = total
        if not first:
            for step in ARRIVAL:
                z_copy(slot, g, step).wait_send()

    def fields_of(slot, g):
        y_copy(slot, g).wait_recv()
        fields = own[g] + got[slot, g].astype(jnp.int32).astype(jnp.float32)
        y_copy(slot, g).wait_send()
        return fields

    def update(k, slot, g):
        fields = fields_of(slot, g)
        beta = beta_col_ref[pl.ds(pl.multiple_of(rep * rep_dev + g * rows, 8), rows), :].astype(jnp.float32)
        later = 1 - slot
        state[later, g, col] = metropolis(
            state[slot, g, col].astype(jnp.float32), fields, slot, color_ref[col],
            noise_buf[k, g * rows:(g + 1) * rows, :], beta,
        )
        for step in ARRIVAL:
            z_copy(later, g, step).start()

    def sweep(k, slot, first=False):
        for g in range(GROUPS):
            matmuls(slot, g, first, False)
        if first:
            noise_copy.wait()
        for g in range(GROUPS):
            update(k, slot, g)

    sweep(0, 0, True)

    def body(k, carry):
        sweep(k, k % 2)
        return carry

    lax.fori_loop(1, sweeps, body, 0)

    for g in range(GROUPS):
        matmuls(0, g, False, True)
    sums = []
    for g in range(GROUPS):
        fields = fields_of(0, g)
        sums.append(jnp.sum(state[0, g, col].astype(jnp.float32) * fields, axis=1, keepdims=True))
    lanes = lax.broadcasted_iota(jnp.int32, (rep_dev, slots), 1)
    ids = rep * rep_dev + lax.broadcasted_iota(jnp.int32, (rep_dev, 1), 0)
    mine = lanes == ids
    total = column_to_row(jnp.concatenate(sums, axis=0), mine)

    stages = (
        (at(row=y_mate),),
        tuple(at(col=z_of(d)) for d in (1, 2, 3)),
        (at(rep=core_mate),),
        (at(rep=x_mate),),
    )
    place = 0
    for number, stage in enumerate(stages):
        esend[number] = jnp.broadcast_to(total, esend.shape[1:])
        copies = []
        for device in stage:
            copies.append(remote(esend.at[number], erecv.at[place], es.at[place], er.at[place], device))
            copies[-1].start()
            place += 1
        if number == 1:
            for g in range(GROUPS):
                for step in (0,) + ARRIVAL:
                    z = z_of(step)
                    x_copy(g, z, step).wait_recv()
                    f_copy(g, z, step).start()
        for offset, copy in enumerate(copies):
            copy.wait_recv()
            total += erecv[place - len(stage) + offset, 0:1, :]
        for copy in copies:
            copy.wait_send()

    mate_ids = partner_ref[pl.ds(pl.multiple_of(rep * rep_dev, 8), rep_dev), :]
    mate = lanes == mate_ids
    betas = beta_row_ref[...].astype(jnp.float32)
    energy_row = -0.5 * total
    mate_energy, energy = picked(mate, energy_row), picked(mine, energy_row)
    swap_gain = (
        (picked(mine, betas) - picked(mate, betas))
        * (energy - mate_energy)
        * (1.0 / (64.0 * spin_count * math.sqrt(spin_count)))
    )
    accept = swap_gain + picked(lanes == jnp.minimum(ids, mate_ids), swap_ref[...]) > 0.0
    scale = 1.0 / (spin_count * math.sqrt(spin_count))
    local = lax.broadcasted_iota(jnp.int32, (rep_dev, rep_dev), 1) == lax.broadcasted_iota(
        jnp.int32, (rep_dev, rep_dev), 0
    )
    energy_ref[...] = column_to_row(jnp.where(accept, mate_energy, energy) * scale, local)
    taken = (lanes == jnp.where(accept, mate_ids, ids)).astype(jnp.float32).astype(jnp.bfloat16)

    for g in range(GROUPS):
        for step in (0,) + ARRIVAL:
            z = z_of(step)
            every[z, rep, g] = state[0, g, z]
            c_copy(g, z, step).wait_recv()
            f_copy(g, z, step).wait_recv()
            x_copy(g, z, step).wait_send()
            c_copy(g, z, step).wait_send()
            f_copy(g, z, step).wait_send()
    for z in range(4):
        out_ref[:, z * piece:(z + 1) * piece] = jnp.dot(
            taken, every[z].reshape(slots, piece), preferred_element_type=jnp.float32
        ).astype(jnp.bfloat16)


def fused(sweeps, spin_count, spin_init, couplings, flip_noise, colors, beta_steps, partners, swap_noise):
    rep_dev, row_width = spin_init.shape
    row_count, _, piece, _ = couplings.shape
    slots = beta_steps.shape[0]
    rows = rep_dev // GROUPS
    block = couplings.astype(F8).reshape(row_count, piece, 4, piece)
    block = jnp.transpose(block, (2, 0, 3, 1))
    vmem = pl.BlockSpec(memory_space=pltpu.VMEM)
    dma = pltpu.SemaphoreType.DMA
    spins_out, energies = pl.pallas_call(
        functools.partial(kernel, sweeps, spin_count),
        out_shape=(
            jax.ShapeDtypeStruct((rep_dev, row_width), jnp.bfloat16),
            jax.ShapeDtypeStruct((1, rep_dev), jnp.float32),
        ),
        in_specs=[vmem, vmem, pl.BlockSpec(memory_space=pl.ANY)] + [vmem] * 5,
        out_specs=(vmem, vmem),
        scratch_shapes=[
            pltpu.VMEM((2, GROUPS, 4, rows, piece), jnp.bfloat16),
            pltpu.VMEM((2, GROUPS, rows, piece), jnp.int16),
            pltpu.VMEM((2, GROUPS, rows, piece), jnp.int16),
            pltpu.VMEM((GROUPS, rows, piece), jnp.float32),
            pltpu.VMEM((sweeps, rep_dev, piece), jnp.float32),
            pltpu.VMEM((4, 4, GROUPS, rows, piece), jnp.bfloat16),
            pltpu.VMEM((4, 8, slots), jnp.float32),
            pltpu.VMEM((6, 8, slots), jnp.float32),
            pltpu.VMEM((8, slots), jnp.float32),
            dma,
            dma((2, GROUPS, 3)), dma((2, GROUPS, 3)),
            dma((2, GROUPS)), dma((2, GROUPS)),
            dma((4, GROUPS)), dma((4, GROUPS)),
            dma((4, GROUPS)), dma((4, GROUPS)),
            dma((4, GROUPS)), dma((4, GROUPS)),
            dma((6,)), dma((6,)),
        ],
        compiler_params=pltpu.CompilerParams(
            collective_id=0, has_side_effects=True, vmem_limit_bytes=56 * 2**20
        ),
    )(
        block, spin_init, flip_noise, colors.reshape(4, 1, piece), beta_steps.reshape(slots, 1),
        beta_steps.reshape(1, slots), partners.reshape(slots, 1), swap_noise.reshape(1, slots),
    )
    return spins_out, energies.reshape(rep_dev)


def general(sweeps, spin_count, spin_init, couplings, flip_noise, colors, beta_steps, partners, swap_noise):
    rep_dev, row_width = spin_init.shape
    col_index = lax.axis_index("col")
    rep_index = lax.axis_index("rep")
    piece_size = row_width // lax.axis_size("col")
    coupling_block = couplings.reshape(-1, row_width)
    own_slots = functools.partial(lax.dynamic_slice_in_dim, start_index=rep_index * rep_dev, slice_size=rep_dev)
    beta_col = own_slots(beta_steps).astype(jnp.float32)[:, None]
    color_part = lax.dynamic_slice_in_dim(colors, col_index * piece_size, piece_size)
    noise_part = lax.dynamic_slice_in_dim(flip_noise, col_index * piece_size, piece_size, 2)

    def partial_fields(spin_state):
        strided = lax.all_gather(spin_state, "row", axis=1, tiled=True)
        return jnp.dot(strided, coupling_block, preferred_element_type=jnp.float32)

    def summed(spin_state):
        return lax.psum_scatter(partial_fields(spin_state), "col", scatter_dimension=1, tiled=True)

    def one_sweep(k, spin_state):
        return metropolis(
            spin_state.astype(jnp.float32), summed(spin_state), k % 2, color_part[None, :], noise_part[k], beta_col
        )

    start = lax.dynamic_slice_in_dim(spin_init, col_index * piece_size, piece_size, 1)
    final = lax.fori_loop(0, sweeps, one_sweep, start)
    final_rows = lax.all_gather(final, "col", axis=1, tiled=True)
    every_spins = lax.all_gather(final_rows, "rep", axis=0, tiled=True)
    energy = -0.5 * lax.psum(jnp.sum(final.astype(jnp.float32) * summed(final), axis=1), ("row", "col"))
    every_energy = lax.all_gather(energy, "rep", axis=0, tiled=True)
    slot_ids = rep_index * rep_dev + jnp.arange(rep_dev, dtype=jnp.int32)
    mate_ids = own_slots(partners)
    all_betas = beta_steps.astype(jnp.float32)
    mate_energy = every_energy[mate_ids]
    swap_gain = (
        (beta_col[:, 0] - all_betas[mate_ids])
        * (energy - mate_energy)
        * (1.0 / (64.0 * spin_count * math.sqrt(spin_count)))
    )
    accept = swap_gain + swap_noise[jnp.minimum(slot_ids, mate_ids)] > 0.0
    spins_out = jnp.where(accept[:, None], every_spins[mate_ids], final_rows)
    energies = jnp.where(accept, mate_energy, energy) * (1.0 / (spin_count * math.sqrt(spin_count)))
    return (spins_out, energies)


def per_device(spin_init, couplings, flip_noise, *others):
    axes = tuple(lax.axis_size(name) for name in ("rep", "row", "col"))
    rep_dev, row_width = spin_init.shape
    sweeps = flip_noise.shape[0]
    fits = axes == (4, 2, 4) and row_width % 512 == 0 and rep_dev % (32 * GROUPS) == 0
    fits = fits and sweeps % 2 == 0 and couplings.shape[0] == 2 and couplings.nbytes <= 2**24
    run = fused if fits else general
    return run(sweeps, row_width * axes[1], spin_init, couplings, flip_noise, *others)


def solution(mesh):
    in_specs = (
        P("rep", "row"),
        P(None, "col", None, "row"),
        P(None, "rep", "row"),
        P("row"),
        P(),
        P(),
        P(),
    )
    out_specs = (P("rep", "row"), P("rep"))
    return jax.shard_map(
        per_device, mesh=mesh, in_specs=in_specs, out_specs=out_specs, check_vma=False
    )
```

```python
import functools
import math

import jax
import jax.numpy as jnp
from jax import lax
from jax.experimental import pallas as pl
from jax.experimental.pallas import tpu as pltpu
from jax.sharding import PartitionSpec as P

GROUPS = 2
F8 = jnp.float8_e4m3fn
ARRIVAL = (1, 3, 2)


def metropolis(values, fields, parity, color_part, noise_part, beta_col):
    energy_cost = beta_col * (values * fields) * (1.0 / 16384.0)
    flipped = (color_part == parity) & (energy_cost < noise_part)
    return jnp.where(flipped, -values, values).astype(jnp.bfloat16)


def column_to_row(column, mask):
    return jnp.sum(jnp.where(mask, column, 0.0), axis=0, keepdims=True)


def picked(mask, row):
    return jnp.sum(jnp.where(mask, row, 0.0), axis=1, keepdims=True)


def kernel(
    sweeps, spin_count, matrix_ref, init_ref, noise_ref, color_ref, beta_col_ref, beta_row_ref,
    partner_ref, swap_ref, out_ref, energy_ref,
    state, part, got, own, noise_buf, every, esend, erecv, esum,
    couple_ref, matrix_buf, matrix_sem, noise_sem, zs, zr, ys, yr, xs, xr, cs, cr, fs, fr, es, er,
):
    rep, row, col = lax.axis_index("rep"), lax.axis_index("row"), lax.axis_index("col")
    rep_dev = init_ref.shape[0]
    piece = matrix_ref.shape[2]
    rows = rep_dev // GROUPS
    slots = beta_row_ref.shape[1]
    y_mate = 1 - row
    core_mate = rep + 1 - 2 * (rep % 2)
    x_mate = rep + 2 - 4 * (rep // 2)

    def at(**changes):
        return (changes.get("rep", rep), changes.get("row", row), changes.get("col", col))

    def z_of(step):
        return (col + step) % 4

    def remote(src, dst, send, recv, device):
        return pltpu.make_async_remote_copy(
            src_ref=src, dst_ref=dst, send_sem=send, recv_sem=recv,
            device_id=device, device_id_type=pl.DeviceIdType.MESH,
        )

    noise_copy = pltpu.make_async_copy(
        noise_ref.at[:, :, pl.ds(pl.multiple_of(col * piece, 128), piece)], noise_buf, noise_sem
    )
    noise_copy.start()

    def matrix_copy(z):
        return pltpu.make_async_copy(
            matrix_ref.at[:, 0, :, pl.ds(z * piece, piece)], matrix_buf.at[z % 2], matrix_sem.at[z % 2]
        )

    matrix_copy(0).start()
    matrix_copy(1).start()

    partners = [at(row=y_mate), at(rep=core_mate), at(rep=x_mate)] + [at(col=z_of(d)) for d in ARRIVAL]
    barrier = pltpu.get_barrier_semaphore()
    for device in partners:
        pl.semaphore_signal(barrier, inc=1, device_id=device, device_id_type=pl.DeviceIdType.MESH)
    pl.semaphore_wait(barrier, len(partners))

    for g in range(GROUPS):
        for z in range(4):
            state[0, g, z] = init_ref[g * rows:(g + 1) * rows, z * piece:(z + 1) * piece]

    tile = 256
    unit = lax.broadcasted_iota(jnp.int32, (tile, tile), 0) == lax.broadcasted_iota(jnp.int32, (tile, tile), 1)
    unit = unit.astype(jnp.float32).astype(jnp.bfloat16)
    for z in range(4):
        matrix_copy(z).wait()

        def turn(index, carry):
            span = pl.ds(pl.multiple_of(index * tile, tile), tile)
            for half in range(2):
                couple_ref[z, half, span, :] = lax.dot_general(
                    unit, matrix_buf[z % 2, half, :, span], (((1,), (1,)), ((), ())),
                    preferred_element_type=jnp.float32,
                ).astype(F8)
            return carry

        lax.fori_loop(0, piece // tile, turn, 0)
        if z < 2:
            matrix_copy(z + 2).start()

    def z_copy(slot, g, step):
        return remote(
            state.at[slot, g, col], state.at[slot, g, col],
            zs.at[slot, g, step - 1], zr.at[slot, g, step - 1], at(col=z_of(step)),
        )

    def y_copy(slot, g):
        return remote(part.at[slot, g], got.at[slot, g], ys.at[slot, g], yr.at[slot, g], at(row=y_mate))

    def product(slot, g, z, half):
        return jnp.dot(
            state[slot, g, z].astype(F8), couple_ref[z, half], preferred_element_type=jnp.float32
        )

    def x_copy(g, z, lane):
        return remote(
            state.at[0, g, z], every.at[z, rep, g], xs.at[lane, g], xr.at[lane, g], at(rep=x_mate)
        )

    def c_copy(g, z, lane):
        return remote(
            state.at[0, g, z], every.at[z, rep, g], cs.at[lane, g], cr.at[lane, g], at(rep=core_mate)
        )

    def f_copy(g, z, lane):
        return remote(
            every.at[z, x_mate, g], every.at[z, x_mate, g], fs.at[lane, g], fr.at[lane, g],
            at(rep=core_mate),
        )

    def matmuls(slot, g, first, last):
        def share(step, lane):
            if last:
                z = z_of(step)
                x_copy(g, z, step).start()
                c_copy(g, z, step).start()

        share(0, 0)
        total = product(slot, g, col, y_mate)
        for step in ARRIVAL:
            if not first:
                z_copy(slot, g, 4 - step).wait_recv()
            share(step, step)
            total += product(slot, g, z_of(step), y_mate)
        part[slot, g] = total.astype(jnp.int32).astype(jnp.int16)
        y_copy(slot, g).start()
        total = product(slot, g, col, row)
        for step in ARRIVAL:
            total += product(slot, g, z_of(step), row)
        own[g] = total
        if not first:
            for step in ARRIVAL:
                z_copy(slot, g, step).wait_send()

    def fields_of(slot, g):
        y_copy(slot, g).wait_recv()
        fields = own[g] + got[slot, g].astype(jnp.int32).astype(jnp.float32)
        y_copy(slot, g).wait_send()
        return fields

    def update(k, slot, g):
        fields = fields_of(slot, g)
        beta = beta_col_ref[pl.ds(pl.multiple_of(rep * rep_dev + g * rows, 8), rows), :].astype(jnp.float32)
        later = 1 - slot
        state[later, g, col] = metropolis(
            state[slot, g, col].astype(jnp.float32), fields, slot, color_ref[col],
            noise_buf[k, g * rows:(g + 1) * rows, :], beta,
        )
        for step in ARRIVAL:
            z_copy(later, g, step).start()

    def sweep(k, slot, first=False):
        for g in range(GROUPS):
            matmuls(slot, g, first, False)
        if first:
            noise_copy.wait()
        for g in range(GROUPS):
            update(k, slot, g)

    sweep(0, 0, True)

    def body(k, carry):
        sweep(k, k % 2)
        return carry

    lax.fori_loop(1, sweeps, body, 0)

    for g in range(GROUPS):
        matmuls(0, g, False, True)
    sums = []
    for g in range(GROUPS):
        fields = fields_of(0, g)
        sums.append(jnp.sum(state[0, g, col].astype(jnp.float32) * fields, axis=1, keepdims=True))
    lanes = lax.broadcasted_iota(jnp.int32, (rep_dev, slots), 1)
    ids = rep * rep_dev + lax.broadcasted_iota(jnp.int32, (rep_dev, 1), 0)
    mine = lanes == ids
    total = column_to_row(jnp.concatenate(sums, axis=0), mine)

    stages = (
        (at(row=y_mate),),
        tuple(at(col=z_of(d)) for d in (1, 2, 3)),
        (at(rep=core_mate),),
        (at(rep=x_mate),),
    )
    place = 0
    for number, stage in enumerate(stages):
        esend[number] = jnp.broadcast_to(total, esend.shape[1:])
        copies = []
        for device in stage:
            copies.append(remote(esend.at[number], erecv.at[place], es.at[place], er.at[place], device))
            copies[-1].start()
            place += 1
        if number == 1:
            for g in range(GROUPS):
                for step in (0,) + ARRIVAL:
                    z = z_of(step)
                    x_copy(g, z, step).wait_recv()
                    f_copy(g, z, step).start()
        for offset, copy in enumerate(copies):
            copy.wait_recv()
            total += erecv[place - len(stage) + offset, 0:1, :]
        for copy in copies:
            copy.wait_send()

    mate_ids = partner_ref[pl.ds(pl.multiple_of(rep * rep_dev, 8), rep_dev), :]
    mate = lanes == mate_ids
    betas = beta_row_ref[...].astype(jnp.float32)
    energy_row = -0.5 * total
    mate_energy, energy = picked(mate, energy_row), picked(mine, energy_row)
    swap_gain = (
        (picked(mine, betas) - picked(mate, betas))
        * (energy - mate_energy)
        * (1.0 / (64.0 * spin_count * math.sqrt(spin_count)))
    )
    accept = swap_gain + picked(lanes == jnp.minimum(ids, mate_ids), swap_ref[...]) > 0.0
    scale = 1.0 / (spin_count * math.sqrt(spin_count))
    local = lax.broadcasted_iota(jnp.int32, (rep_dev, rep_dev), 1) == lax.broadcasted_iota(
        jnp.int32, (rep_dev, rep_dev), 0
    )
    energy_ref[...] = column_to_row(jnp.where(accept, mate_energy, energy) * scale, local)
    taken = (lanes == jnp.where(accept, mate_ids, ids)).astype(jnp.float32).astype(jnp.bfloat16)

    for g in range(GROUPS):
        for step in (0,) + ARRIVAL:
            z = z_of(step)
            every[z, rep, g] = state[0, g, z]
            c_copy(g, z, step).wait_recv()
            f_copy(g, z, step).wait_recv()
            x_copy(g, z, step).wait_send()
            c_copy(g, z, step).wait_send()
            f_copy(g, z, step).wait_send()
    for z in range(4):
        out_ref[:, z * piece:(z + 1) * piece] = jnp.dot(
            taken, every[z].reshape(slots, piece), preferred_element_type=jnp.float32
        ).astype(jnp.bfloat16)


def fused(sweeps, spin_count, spin_init, couplings, flip_noise, colors, beta_steps, partners, swap_noise):
    rep_dev, row_width = spin_init.shape
    row_count, _, piece, _ = couplings.shape
    slots = beta_steps.shape[0]
    rows = rep_dev // GROUPS
    vmem = pl.BlockSpec(memory_space=pltpu.VMEM)
    hbm = pl.BlockSpec(memory_space=pl.ANY)
    dma = pltpu.SemaphoreType.DMA
    spins_out, energies = pl.pallas_call(
        functools.partial(kernel, sweeps, spin_count),
        out_shape=(
            jax.ShapeDtypeStruct((rep_dev, row_width), jnp.bfloat16),
            jax.ShapeDtypeStruct((1, rep_dev), jnp.float32),
        ),
        in_specs=[hbm, vmem, hbm] + [vmem] * 5,
        out_specs=(vmem, vmem),
        scratch_shapes=[
            pltpu.VMEM((2, GROUPS, 4, rows, piece), jnp.bfloat16),
            pltpu.VMEM((2, GROUPS, rows, piece), jnp.int16),
            pltpu.VMEM((2, GROUPS, rows, piece), jnp.int16),
            pltpu.VMEM((GROUPS, rows, piece), jnp.float32),
            pltpu.VMEM((sweeps, rep_dev, piece), jnp.float32),
            pltpu.VMEM((4, 4, GROUPS, rows, piece), jnp.bfloat16),
            pltpu.VMEM((4, 8, slots), jnp.float32),
            pltpu.VMEM((6, 8, slots), jnp.float32),
            pltpu.VMEM((8, slots), jnp.float32),
            pltpu.VMEM((4, row_count, piece, piece), F8),
            pltpu.VMEM((2, row_count, piece, piece), jnp.bfloat16),
            dma((2,)),
            dma,
            dma((2, GROUPS, 3)), dma((2, GROUPS, 3)),
            dma((2, GROUPS)), dma((2, GROUPS)),
            dma((4, GROUPS)), dma((4, GROUPS)),
            dma((4, GROUPS)), dma((4, GROUPS)),
            dma((4, GROUPS)), dma((4, GROUPS)),
            dma((6,)), dma((6,)),
        ],
        compiler_params=pltpu.CompilerParams(
            collective_id=0, has_side_effects=True, vmem_limit_bytes=56 * 2**20
        ),
    )(
        couplings, spin_init, flip_noise, colors.reshape(4, 1, piece), beta_steps.reshape(slots, 1),
        beta_steps.reshape(1, slots), partners.reshape(slots, 1), swap_noise.reshape(1, slots),
    )
    return spins_out, energies.reshape(rep_dev)


def general(sweeps, spin_count, spin_init, couplings, flip_noise, colors, beta_steps, partners, swap_noise):
    rep_dev, row_width = spin_init.shape
    col_index = lax.axis_index("col")
    rep_index = lax.axis_index("rep")
    piece_size = row_width // lax.axis_size("col")
    coupling_block = couplings.reshape(-1, row_width)
    own_slots = functools.partial(lax.dynamic_slice_in_dim, start_index=rep_index * rep_dev, slice_size=rep_dev)
    beta_col = own_slots(beta_steps).astype(jnp.float32)[:, None]
    color_part = lax.dynamic_slice_in_dim(colors, col_index * piece_size, piece_size)
    noise_part = lax.dynamic_slice_in_dim(flip_noise, col_index * piece_size, piece_size, 2)

    def partial_fields(spin_state):
        strided = lax.all_gather(spin_state, "row", axis=1, tiled=True)
        return jnp.dot(strided, coupling_block, preferred_element_type=jnp.float32)

    def summed(spin_state):
        return lax.psum_scatter(partial_fields(spin_state), "col", scatter_dimension=1, tiled=True)

    def one_sweep(k, spin_state):
        return metropolis(
            spin_state.astype(jnp.float32), summed(spin_state), k % 2, color_part[None, :], noise_part[k], beta_col
        )

    start = lax.dynamic_slice_in_dim(spin_init, col_index * piece_size, piece_size, 1)
    final = lax.fori_loop(0, sweeps, one_sweep, start)
    final_rows = lax.all_gather(final, "col", axis=1, tiled=True)
    every_spins = lax.all_gather(final_rows, "rep", axis=0, tiled=True)
    energy = -0.5 * lax.psum(jnp.sum(final.astype(jnp.float32) * summed(final), axis=1), ("row", "col"))
    every_energy = lax.all_gather(energy, "rep", axis=0, tiled=True)
    slot_ids = rep_index * rep_dev + jnp.arange(rep_dev, dtype=jnp.int32)
    mate_ids = own_slots(partners)
    all_betas = beta_steps.astype(jnp.float32)
    mate_energy = every_energy[mate_ids]
    swap_gain = (
        (beta_col[:, 0] - all_betas[mate_ids])
        * (energy - mate_energy)
        * (1.0 / (64.0 * spin_count * math.sqrt(spin_count)))
    )
    accept = swap_gain + swap_noise[jnp.minimum(slot_ids, mate_ids)] > 0.0
    spins_out = jnp.where(accept[:, None], every_spins[mate_ids], final_rows)
    energies = jnp.where(accept, mate_energy, energy) * (1.0 / (spin_count * math.sqrt(spin_count)))
    return (spins_out, energies)


def per_device(spin_init, couplings, flip_noise, *others):
    axes = tuple(lax.axis_size(name) for name in ("rep", "row", "col"))
    rep_dev, row_width = spin_init.shape
    sweeps = flip_noise.shape[0]
    fits = axes == (4, 2, 4) and row_width % 1024 == 0 and rep_dev % (32 * GROUPS) == 0
    fits = fits and sweeps % 2 == 0 and couplings.shape[0] == 2 and couplings.nbytes <= 2**24
    run = fused if fits else general
    return run(sweeps, row_width * axes[1], spin_init, couplings, flip_noise, *others)


def solution(mesh):
    in_specs = (
        P("rep", "row"),
        P(None, "col", None, "row"),
        P(None, "rep", "row"),
        P("row"),
        P(),
        P(),
        P(),
    )
    out_specs = (P("rep", "row"), P("rep"))
    return jax.shard_map(
        per_device, mesh=mesh, in_specs=in_specs, out_specs=out_specs, check_vma=False
    )
```
